128 devices in a mesh: seq: 32 (over z, x, y_hi), tp: 4 (over y_lo, core).
Axes of the slice: x: 4, y: 4 (y_hi: 2, y_lo: 2; y = y_hi * 2 + y_lo), z: 4, core: 2. Of those that a mesh axis runs over, the one named last changes fastest.
Arguments:
- attn_out: bfloat16 [10240, 8192], P('seq', 'tp'), may hold values from -6 to 6
- out_weight: bfloat16 [8192, 8192], P('tp', 'seq'), may hold values from -0.0625 to 0.0625
- residual: bfloat16 [10240, 8192], P(('seq', 'tp')), may hold values from -114.6116 to 114.6116
- norm_gain: float32 [8192], replicated, may hold values from 0.5 to 1.5
- kv_weight: bfloat16 [8192, 2, 1024], P(None, None, 'tp'), may hold values from -0.0625 to 0.0625
Outputs:
- residual_out: bfloat16 [10240, 8192], P(('seq', 'tp'))
- quantized: bfloat16 [10240, 8192], P(('seq', 'tp'))
- peak: float32 [], replicated
- key_value: bfloat16 [10240, 2, 1024], P('seq', None, 'tp')
The draws below stay inside these ranges and needn't reach their ends.
All inputs are finite; a program needn't handle non-finite values. Where the reference program divides by a largest or mean magnitude, that divisor is 1e-20 or more.
Results may differ from the reference program's by a relative error of at most 0.014.
Values may be sent and summed in bfloat16 or wider, within the bound.
No kernel may reach another device: no remote copies, remote signals or barrier semaphores. Data moves between devices by JAX's collectives and lax.ppermute only.
A program may use at most 128 MiB of HBM per device.

```python
import jax
import jax.numpy as jnp
from jax import lax

D = 8192
KVD = 1024
TOKENS = 10240
N_TP = 4


def draw_residual(key, part):
    first_key = jax.random.fold_in(key, 11)
    second_key = jax.random.fold_in(key, 12)
    third_key = jax.random.fold_in(key, 13)
    base = jnp.clip(jax.random.normal(first_key, (TOKENS, D), jnp.float32), -6.0, 6.0)
    low_end = 0.2
    high_end = 1.2
    column = jax.random.randint(second_key, (TOKENS,), 0, D)
    signs = (jax.random.randint(third_key, (TOKENS,), 0, 2) * 2 - 1).astype(jnp.float32)
    ramp = jnp.arange(TOKENS, dtype=jnp.float32) / max(TOKENS - 1, 1)
    magnitude = low_end * (high_end / low_end) ** ramp * D ** 0.5
    places = (jnp.arange(D)[None, :] == column[:, None]).astype(jnp.float32)
    return (base + places * (signs * magnitude)[:, None]).astype(jnp.bfloat16)


def shard_levels(own_key, shape, split, smallest, largest):
    factor_of, own = 1.0, jax.random.fold_in(own_key, 6)
    for axis_at, blocks in split:
        draws = jnp.exp(jax.random.uniform(jax.random.fold_in(own, axis_at), (blocks,), jnp.float32, smallest / len(split), largest / len(split)))
        factor_of = factor_of * jnp.repeat(draws, shape[axis_at] // blocks).reshape([-1 if axis == axis_at else 1 for axis in range(len(shape))])
    return factor_of


def normal_values(stream_key, extent, deviation, bound, cuts=(), held_as=jnp.bfloat16):
    entries = jax.random.normal(stream_key, extent, jnp.float32) * deviation
    if len(cuts) > 0:
        entries = shard_levels(stream_key, extent, cuts, -0.22, 0.18) * entries
    return jnp.clip(entries, min=-bound, max=bound).astype(held_as)


def setup_inputs(seed: int = 0) -> dict:
    keys = jax.random.split(jax.random.key(seed), 6)
    return {
        "attn_out": normal_values(keys[0], (TOKENS, D), 1.0, 6.0, ((0, 32), (1, 4))),
        "out_weight": normal_values(keys[1], (D, D), D ** -0.5, 0.0625, ((0, 4), (1, 32))),
        "residual": draw_residual(jax.random.fold_in(keys[5], 71), 0),
        "norm_gain": jnp.clip(1.0 + 0.1 * jax.random.normal(keys[3], (D,), jnp.float32), 0.5, 1.5),
        "kv_weight": normal_values(keys[4], (D, 2, KVD), D ** -0.5, 0.0625, ((2, 4),)),
    }


def reference(attn_out, out_weight, residual, norm_gain, kv_weight):
    group_width = D // N_TP
    summed = jnp.zeros((TOKENS, D), jnp.float32)
    for group_index in range(N_TP):
        lower = group_index * group_width
        partial_value = jnp.dot(attn_out[:, lower:lower + group_width], out_weight[lower:lower + group_width, :], preferred_element_type=jnp.float32)
        summed = summed + lax.optimization_barrier(partial_value.astype(jnp.bfloat16)).astype(jnp.float32)
    hidden = residual.astype(jnp.float32) + summed
    mean_square = lax.optimization_barrier(jnp.mean(hidden * hidden, axis=1, keepdims=True))
    normed = (hidden * lax.rsqrt(mean_square + 1e-05) * norm_gain).astype(jnp.bfloat16)
    peak_value = jnp.max(jnp.abs(normed.astype(jnp.float32)))
    quantized = (normed.astype(jnp.float32) * (448.0 / peak_value)).astype(jnp.bfloat16)
    projected = jnp.dot(quantized, kv_weight.reshape(D, 2 * KVD), preferred_element_type=jnp.float32)
    key_value = (projected * (peak_value / 448.0)).astype(jnp.bfloat16).reshape(TOKENS, 2, KVD)
    return (hidden.astype(jnp.bfloat16), quantized, peak_value, key_value)
```

```python
import functools

import jax
import jax.numpy as jnp
from jax import lax
from jax.experimental import pallas as pl
from jax.experimental.pallas import tpu as pltpu
from jax.sharding import Mesh
from jax.sharding import PartitionSpec as P

SEQ = ("z", "x", "h")
TP = ("l", "c")
SEQ_TP = SEQ + TP
BF = jnp.bfloat16
F32 = jnp.float32
VMEM_SPEC = pl.BlockSpec(memory_space=pltpu.VMEM)
SMEM_SPEC = pl.BlockSpec(memory_space=pltpu.SMEM)


def from_peer(value, axis, step):
    size = lax.axis_size(axis)
    return lax.ppermute(value, axis, [(i, (i - step) % size) for i in range(size)])


def partial_products(tokens, weights):
    n_t, n_w = len(tokens), len(weights)
    half = tokens[0].shape[0] // 2
    wide = weights[0][0].shape[1]

    def body(*refs):
        t_refs, w_refs = refs[:n_t], refs[n_t : n_t + 2 * n_w]
        keep, send = refs[n_t + 2 * n_w :]
        for t in range(n_t):
            for w in range(n_w):
                upper, lower = w_refs[2 * w], w_refs[2 * w + 1]
                depth = upper.shape[0]
                acc = jnp.dot(t_refs[t][:, :depth], upper[...], preferred_element_type=F32)
                acc += jnp.dot(t_refs[t][:, depth:], lower[...], preferred_element_type=F32)
                rounded = acc.astype(BF)
                keep[t, :, w * wide : (w + 1) * wide] = rounded[:half]
                send[t, :, w * wide : (w + 1) * wide] = rounded[half:]

    shape = jax.ShapeDtypeStruct((n_t, half, n_w * wide), BF)
    flat = [piece for pair in weights for piece in pair]
    flops = 2 * n_t * tokens[0].shape[0] * tokens[0].shape[1] * n_w * wide
    return pl.pallas_call(
        body,
        out_shape=(shape, shape),
        in_specs=[VMEM_SPEC] * (n_t + 2 * n_w),
        out_specs=(VMEM_SPEC, VMEM_SPEC),
        cost_estimate=pl.CostEstimate(flops=flops, bytes_accessed=0, transcendentals=0),
        name="partial_products",
    )(*tokens, *flat)


def norm_rows(place, pieces, residual, gain, layout):
    rows, width = residual.shape
    n_p = len(pieces)
    block = width // 32

    def body(place_ref, *refs):
        p_refs = refs[:n_p]
        res_ref, gain_ref, out_ref, normed_ref, peak_ref, hidden = refs[n_p:]
        z, x, h = place_ref[0], place_ref[1], place_ref[2]
        total = jnp.zeros((rows, block), F32)
        for p, (dx, blocks) in enumerate(layout):
            for at, (dz, dh) in enumerate(blocks):
                where = ((((z + dz) & 3) * 4 + ((x + dx) & 3)) * 2 + (h ^ dh)) * block
                where = pl.multiple_of(where, block)
                value = p_refs[p][:, at * block : (at + 1) * block].astype(F32)
                value += res_ref[:, pl.ds(where, block)].astype(F32)
                out_ref[:, pl.ds(where, block)] = value.astype(BF)
                hidden[:, pl.ds(where, block)] = value
                total += value * value
        scale = lax.rsqrt(jnp.sum(total, axis=1, keepdims=True) / width + 1e-05)
        most = jnp.zeros((rows, block), F32)
        for b in range(32):
            span = slice(b * block, (b + 1) * block)
            normed = (hidden[:, span] * scale * gain_ref[:, span]).astype(BF)
            normed_ref[:, span] = normed
            most = jnp.maximum(most, jnp.abs(normed.astype(F32)))
        folded = jnp.maximum(most[:, :128], most[:, 128:])
        peak_ref[...] = jnp.max(folded.reshape(rows // 8, 8, 128), axis=0)

    return pl.pallas_call(
        body,
        out_shape=(
            jax.ShapeDtypeStruct((rows, width), BF),
            jax.ShapeDtypeStruct((rows, width), BF),
            jax.ShapeDtypeStruct((8, 128), F32),
        ),
        in_specs=[SMEM_SPEC] + [VMEM_SPEC] * (n_p + 2),
        out_specs=(VMEM_SPEC,) * 3,
        scratch_shapes=[pltpu.VMEM((rows, width), F32)],
        cost_estimate=pl.CostEstimate(flops=8 * rows * width, bytes_accessed=0, transcendentals=0),
        name="norm_rows",
    )(place, *pieces, residual, gain.reshape(1, width))


def over_axis(value, axis):
    size = lax.axis_size(axis)
    best = value
    for step in range(1, size):
        best = jnp.maximum(best, from_peer(value, axis, step))
    return best


def spread(value, axis, split):
    upper, lower = value
    up_m, lo_p = from_peer(upper, axis, -1), from_peer(lower, axis, 1)
    lo_m, up_p = from_peer(lower, axis, -1), from_peer(upper, axis, 1)
    up_2, lo_2 = from_peer(up_m, axis, -1), from_peer(lo_p, axis, 1)
    return {0: (upper, lower), 3: (up_m, lo_m), 1: (up_p, lo_p), 2: (up_2, lo_2)}


def per_device(attn_out, out_weight, residual, norm_gain, kv_weight):
    z, x, h, l, c = (lax.axis_index(a) for a in SEQ_TP)
    n_tok, depth = attn_out.shape
    rows, width = residual.shape
    kv_cols = kv_weight.shape[2]

    quarters = attn_out.reshape(2, 2, rows, depth)

    def quarter(dc, dl):
        return lax.dynamic_slice(quarters, (l ^ dl, c ^ dc, 0, 0), (1, 1, rows, depth)).reshape(
            rows, depth
        )

    tokens_own = (
        jnp.concatenate([quarter(0, 0), quarter(0, 1)], axis=0),
        jnp.concatenate([quarter(1, 0), quarter(1, 1)], axis=0),
    )
    weight_own = (out_weight[: depth // 2], out_weight[depth // 2 :])
    weight_pair = tuple(from_peer(piece, "h", 1) for piece in weight_own)
    w_own = spread(weight_own, "z", 0)
    tok = spread(tokens_own, "x", 0)
    w_pair = spread(weight_pair, "z", 0)
    kv_flat = kv_weight.reshape(width, 2 * kv_cols)

    order = (0, 1, 3, 2)
    tokens = [jnp.concatenate(tok[dx], axis=0) for dx in order]
    groups = [
        [(0, 0), (1, 0), (3, 0), (0, 1), (2, 0)],
        [(1, 1), (3, 1)],
        [(2, 1)],
    ]
    pieces, layout = [], []
    for blocks in groups:
        weights = [(w_pair if dh else w_own)[dz] for dz, dh in blocks]
        keep, send = partial_products(tokens, weights)
        got = from_peer(send, "c", 1)
        both = keep.astype(F32) + got.astype(F32)
        got = from_peer(both[:, rows:].astype(BF), "l", 1)
        summed = both[:, :rows] + got.astype(F32)
        for at, dx in enumerate(order):
            part = summed[at]
            if dx:
                part = from_peer(part.astype(BF), "x", -dx)
            pieces.append(part)
            layout.append(((-dx) % 4, blocks))
    place = jnp.stack([z, x, h]).astype(jnp.int32)
    residual_out, normed, most = norm_rows(place, pieces, residual, norm_gain, layout)

    across = from_peer(normed, "l", 1)
    normed_near = from_peer(normed, "c", 1)
    normed_far = from_peer(across, "c", 1)
    near = jnp.dot(
        jnp.concatenate([normed, normed_near], axis=0), kv_flat, preferred_element_type=F32
    ).astype(BF)
    far = jnp.dot(
        jnp.concatenate([across, normed_far], axis=0), kv_flat, preferred_element_type=F32
    ).astype(BF)
    for axis in ("c", "l", "h", "x", "z"):
        most = over_axis(most, axis)
    peak_value = jnp.max(most)
    quantized = (normed.astype(F32) * (448.0 / peak_value)).astype(BF)

    def in_order(block, flip):
        a, b = block[:rows], block[rows:]
        return jnp.concatenate([jnp.where(flip, b, a), jnp.where(flip, a, b)], axis=0)

    near, far = in_order(near, c == 1), in_order(far, c == 1)
    key_value = jnp.concatenate(
        [jnp.where(l == 1, far, near), jnp.where(l == 1, near, far)], axis=0
    ).reshape(n_tok, 2, kv_cols)
    return (residual_out, quantized, peak_value, key_value)


def solution(mesh):
    finer = Mesh(mesh.devices.reshape(4, 4, 2, 2, 2), SEQ_TP)
    in_specs = (P(SEQ, TP), P(TP, SEQ), P(SEQ_TP, None), P(), P(None, None, TP))
    out_specs = (P(SEQ_TP, None), P(SEQ_TP, None), P(), P(SEQ, None, TP))
    return jax.shard_map(
        per_device, mesh=finer, in_specs=in_specs, out_specs=out_specs, check_vma=False
    )
```
